128 devices in a mesh: seq: 8 (over y, core), chan: 16 (over z, x).
Axes of the slice: x: 4, y: 4, z: 4, core: 2. Of those that a mesh axis runs over, the one named last changes fastest.
Arguments:
- scan_input: bfloat16 [2048, 5120], P('seq', 'chan'), may hold values from -6 to 6
- gate_input: bfloat16 [2048, 5120], P('seq', 'chan'), may hold values from -6 to 6
- step_raw: bfloat16 [2048, 5120], P('seq', 'chan')
- log_rates: float32 [16, 5120], P(None, 'chan')
- skip_gain: float32 [5120], P('chan'), may hold values from 0.5 to 1.5
- state_write: float32 [16, 2048], P(None, 'seq'), may hold values from -6 to 6
- state_read: float32 [16, 2048], P(None, 'seq'), may hold values from -6 to 6
- out_weight: bfloat16 [5120, 2560], P('chan'), may hold values from -0.078125 to 0.078125
- out_cotangent: bfloat16 [2048, 2560], P('seq', 'chan'), may hold values from -6 to 6
Outputs:
- grad_input: bfloat16 [2048, 5120], P('seq', 'chan')
- grad_gate: bfloat16 [2048, 5120], P('seq', 'chan')
- grad_step: bfloat16 [2048, 5120], P('seq', 'chan')
- grad_rates: float32 [16, 5120], P(None, 'chan')
- grad_skip: float32 [5120], P('chan')
- grad_write: float32 [16, 2048], P(None, ('seq', 'chan'))
- grad_read: float32 [16, 2048], P(None, ('seq', 'chan'))
- grad_weight: float32 [5120, 2560], P('chan', 'seq')
The draws below stay inside these ranges and needn't reach their ends.
All inputs are finite; a program needn't handle non-finite values.
Results may differ from the reference program's by a relative error of at most 0.0095.
Values may be sent and summed in bfloat16 or wider, within the bound.
A program may use at most 64 MiB of HBM per device.

```python
import jax
import jax.numpy as jnp
from jax import lax

DM = 2560
EI = 5120
DS = 16
TOKENS = 2048
N_CHAN = 16


def draw_log_rates(key, part):
    first, second = jax.random.split(key, 2)
    root = jnp.sqrt(jnp.float32(TOKENS))
    share = 0.5
    quick = jax.random.uniform(first, (DS, EI), jnp.float32) < share
    spread = jax.random.uniform(second, (DS, EI), jnp.float32)
    slow_rate = 0.2 / root * jnp.power(10.0, spread)
    quick_rate = root / 40.0 * jnp.power(10.0, spread)
    return jnp.log(jnp.where(quick, quick_rate, slow_rate)).astype(jnp.float32)


def draw_step_raw(key, part):
    root = jnp.sqrt(jnp.float32(TOKENS))
    spread = jax.random.uniform(key, (TOKENS, EI), jnp.float32)
    target = 0.3 * jnp.power(10.0, spread) / root
    return jnp.log(jnp.expm1(target)).astype(jnp.bfloat16)


def with_spikes(values, stream_key, source, target, shards_of, factor):
    owner, partner = [(jnp.arange(values.shape[dim]) // (values.shape[dim] // shards_of)).reshape([-1 if axis == dim else 1 for axis in range(values.ndim)]) for dim in (source, target)]
    chosen = jax.random.permutation(stream_key, shards_of)[partner]
    strong = (owner == chosen) | (owner == (partner + shards_of // 2) % shards_of)
    return jnp.where(strong, factor * values, values)


def levels(stream_key, dims, cuts, least, largest):
    factor_of, own = 1.0, jax.random.fold_in(stream_key, 6)
    for position, parts in cuts:
        steps = jnp.exp(jax.random.uniform(jax.random.fold_in(own, position), (parts,), jnp.float32, least / len(cuts), largest / len(cuts)))
        factor_of = factor_of * jnp.repeat(steps, dims[position] // parts).reshape([-1 if axis == position else 1 for axis in range(len(dims))])
    return factor_of


def bell_draw(rng, extent, scale, most, cuts=(), kind=jnp.bfloat16):
    result = scale * jax.random.normal(rng, extent, jnp.float32)
    if cuts:
        result = result * levels(rng, extent, cuts, -0.22, 0.18)
    return jnp.clip(result, -most, most).astype(kind)


def bell_draw_with(own_key, shape, scale, limit, shards, heavy, kind=jnp.bfloat16):
    entries = scale * jax.random.normal(own_key, shape, jnp.float32)
    if shards:
        entries = entries * levels(own_key, shape, shards, -0.22, 0.18)
    return jnp.clip(with_spikes(entries, jax.random.fold_in(own_key, 3), *heavy), -limit, limit).astype(kind)


def setup_inputs(seed: int = 0) -> dict:
    key_list = jax.random.split(jax.random.key(seed), 10)
    return {
        "scan_input": bell_draw_with(key_list[0], (TOKENS, EI), 1.0, 6.0, ((0, 8), (1, 16)), (1, 0, 16, 2.0)),
        "gate_input": bell_draw(key_list[1], (TOKENS, EI), 1.0, 6.0, ((0, 8), (1, 16))),
        "step_raw": draw_step_raw(jax.random.fold_in(key_list[9], 71), 0),
        "log_rates": draw_log_rates(jax.random.fold_in(key_list[9], 71), 0),
        "skip_gain": jnp.clip(1.0 + 0.1 * jax.random.normal(key_list[4], (EI,), jnp.float32), 0.5, 1.5),
        "state_write": bell_draw(key_list[5], (DS, TOKENS), 1.0, 6.0, ((1, 8),), jnp.float32),
        "state_read": bell_draw(key_list[6], (DS, TOKENS), 1.0, 6.0, ((1, 8),), jnp.float32),
        "out_weight": bell_draw(key_list[7], (EI, DM), EI ** -0.5, 0.078125, ((0, 16),)),
        "out_cotangent": bell_draw_with(key_list[8], (TOKENS, DM), 1.0, 6.0, ((0, 8), (1, 16)), (0, 1, 16, 2.0)),
    }


def reference(scan_input, gate_input, step_raw, log_rates, skip_gain, state_write, state_read, out_weight, out_cotangent):
    width = EI // N_CHAN
    delta = jax.nn.softplus(step_raw.astype(jnp.float32))
    a_neg = -jnp.exp(log_rates)
    xf = scan_input.astype(jnp.float32)
    zf = gate_input.astype(jnp.float32)
    gate_sig = jax.nn.sigmoid(zf)
    gate_silu = zf * gate_sig
    dg = jnp.dot(out_cotangent, out_weight.T, preferred_element_type=jnp.float32)
    dy = dg * gate_silu
    b_rows = state_write.T
    c_rows = state_read.T

    def group(index):
        start = index * width
        x_g = lax.dynamic_slice_in_dim(xf, start, width, 1)
        d_g = lax.dynamic_slice_in_dim(delta, start, width, 1)
        a_g = lax.dynamic_slice_in_dim(a_neg, start, width, 1)
        dy_g = lax.dynamic_slice_in_dim(dy, start, width, 1)
        skip_g = lax.dynamic_slice_in_dim(skip_gain, start, width, 0)

        def forward(state, inputs):
            d_t, x_t, b_t = inputs
            state = jnp.exp(d_t[None, :] * a_g) * state + b_t[:, None] * (d_t * x_t)[None, :]
            return state, state

        zero_state = jnp.zeros((DS, width), jnp.float32)
        _, states = lax.scan(forward, zero_state, (d_g, x_g, b_rows))
        y_g = jnp.einsum("nt,tne->te", state_read, states) + skip_g[None, :] * x_g
        grad_c_part = jnp.einsum("te,tne->nt", dy_g, states)
        previous = jnp.concatenate([zero_state[None], states[:-1]], axis=0)

        def backward(carry, inputs):
            omega, acc = carry
            d_t, x_t, b_t, c_t, dy_t, prev_t = inputs
            dec = jnp.exp(d_t[None, :] * a_g)
            lam = c_t[:, None] * dy_t[None, :] + omega
            lam_b = jnp.sum(lam * b_t[:, None], axis=0)
            gdelta = x_t * lam_b + jnp.sum(lam * a_g * dec * prev_t, axis=0)
            gx = d_t * lam_b + dy_t * skip_g
            gb = jnp.sum(lam * (d_t * x_t)[None, :], axis=1)
            acc = acc + lam * prev_t * dec * d_t[None, :]
            return (dec * lam, acc), (gx, gdelta, gb)

        (_, grad_a), (gx_g, gdelta_g, gb_rows) = lax.scan(
            backward, (zero_state, zero_state), (d_g, x_g, b_rows, c_rows, dy_g, previous), reverse=True)
        return y_g, gx_g, gdelta_g, grad_a, gb_rows.T, grad_c_part

    outs = lax.map(group, jnp.arange(N_CHAN, dtype=jnp.int32))
    y_all, gx_all, gdelta_all, grad_a_all, gb_all, gc_all = outs

    def join(stack):
        return jnp.transpose(stack, (1, 0, 2)).reshape(stack.shape[1], EI)

    y = join(y_all)
    grad_input = join(gx_all).astype(jnp.bfloat16)
    grad_delta = join(gdelta_all)
    grad_a = jnp.transpose(grad_a_all, (1, 0, 2)).reshape(DS, EI)
    grad_rates = grad_a * a_neg
    grad_write = jnp.sum(gb_all, axis=0)
    grad_read = jnp.sum(gc_all, axis=0)
    grad_skip = jnp.sum(dy * xf, axis=0)
    gated = (y * gate_silu).astype(jnp.bfloat16)
    grad_weight = jnp.dot(gated.T, out_cotangent, preferred_element_type=jnp.float32)
    grad_gate = (dg * y * gate_sig * (1.0 + zf * (1.0 - gate_sig))).astype(jnp.bfloat16)
    grad_step = (grad_delta * jax.nn.sigmoid(step_raw.astype(jnp.float32))).astype(jnp.bfloat16)
    return (grad_input, grad_gate, grad_step, grad_rates, grad_skip, grad_write, grad_read, grad_weight)
```

```python
import functools
import math

import jax
import jax.numpy as jnp
from jax import lax
from jax.experimental import pallas as pl
from jax.experimental.pallas import tpu as pltpu
from jax.sharding import PartitionSpec as P

F32, BF16 = jnp.float32, jnp.bfloat16
LOG2E, LN2 = 1.0 / math.log(2.0), math.log(2.0)
T, E, PAD, NS, DM = 256, 320, 384, 16, 2560
SUB, STEPS = 8, 32
FEAT = 160
UNROLL = 2


def sigmoid(v):
    return 1.0 / (1.0 + jnp.exp(-v))


def kernel(
    x_ref, z_ref, st_ref, lr_ref, sk_ref, b_ref, c_ref, w_hbm, do_ref,
    gi_ref, gg_ref, gs_ref, gr_ref, gk_ref, gwrite_ref, gread_ref, gw_ref,
    W, G, GP, DOP, XP, ZP, TP, SKP, LRP, A2N, A2B, BP, BTN, BTP, BB, D, DX, DY, Y, LB, GD,
    DEC, HS, HPRE, HIN, PW, CS, YN, GF, GT, GTP, DGT, DG, PB, SB, RB, XF, XB, XR, R2, GX,
    w_sem, g_send, g_recv, p_send, p_recv, f_send, f_recv, b_send, b_recv, r_send, r_recv,
    n_send, n_recv, x_send, x_recv,
):
    s, c = lax.axis_index("seq"), lax.axis_index("chan")
    kap, chip = s % 2, s // 2
    partner = s + 1 - 2 * kap
    up, down = ((chip + 1) % 4) * 2 + kap, ((chip + 3) % 4) * 2 + kap

    def rc(src, dst, ss, rs, ps, pc):
        return pltpu.make_async_remote_copy(
            src_ref=src, dst_ref=dst, send_sem=ss, recv_sem=rs,
            device_id=(ps, pc), device_id_type=pl.DeviceIdType.MESH,
        )

    w_copy = pltpu.make_async_copy(w_hbm, W, w_sem)
    w_copy.start()
    barrier = pltpu.get_barrier_semaphore()
    for o in range(1, 16):
        pl.semaphore_signal(barrier, inc=1, device_id=(s, (c + o) % 16), device_id_type=pl.DeviceIdType.MESH)
    for o in range(1, 8):
        pl.semaphore_signal(barrier, inc=1, device_id=((s + o) % 8, c), device_id_type=pl.DeviceIdType.MESH)

    DOP[:, FEAT:] = jnp.zeros((T, 256 - FEAT), BF16)
    DOP[:, :FEAT] = do_ref[...]
    own = pl.multiple_of(c * FEAT, 32)
    for tb in range(2):
        rows = slice(128 * tb, 128 * tb + 128)
        first = DOP[rows, :128].astype(F32).T.astype(BF16)
        second = DOP[rows, 128:].astype(F32).T.astype(BF16)
        G[pl.ds(own, 128), rows] = first
        G[pl.ds(own + 128, FEAT - 128), rows] = second[: FEAT - 128]
    pl.semaphore_wait(barrier, 22)

    def g_copy(o):
        q = pl.ds(own, FEAT)
        return rc(G.at[q], G.at[q], g_send.at[o], g_recv.at[o], s, (c + o) % 16)

    gathers = [g_copy(o) for o in range(1, 16)]
    for copy in gathers:
        copy.start()

    for src, dst in ((x_ref, XP), (z_ref, ZP), (st_ref, TP)):
        dst[:, 256:] = jnp.zeros((T, 128), BF16)
        dst[:, :E] = src[...]
    SKP[:, 256:] = jnp.zeros((8, 128), F32)
    SKP[0:1, :E] = sk_ref[...]
    LRP[:, 256:] = jnp.zeros((NS, 128), F32)
    LRP[:, :E] = lr_ref[...]
    for j in range(3):
        A2N[j] = -LOG2E * jnp.exp(LRP[:, 128 * j : 128 * j + 128])
    for n in range(NS):
        for j in range(3):
            tt = (n % 4) * 3 + j
            A2B[n // 4, 8 * tt : 8 * tt + 8, :] = jnp.broadcast_to(A2N[j, n : n + 1, :], (8, 128))

    def lanes(j):
        return slice(128 * j, 128 * j + 128)

    def perm(m, half, j):
        return pl.ds(j * T + 8 * (16 * (m % 2) + 8 * half) + m // 2, 8, stride=8)

    def prologue(m, carry):
        rows = pl.ds(pl.multiple_of(16 * m, 16), 16)
        for j in range(3):
            st = TP[rows, lanes(j)].astype(F32)
            delta = jnp.maximum(st, 0.0) + jnp.log1p(jnp.exp(-jnp.abs(st)))
            dx = delta * XP[rows, lanes(j)].astype(F32)
            for half in range(2):
                D[perm(m, half, j), :] = delta[8 * half : 8 * half + 8]
                DX[perm(m, half, j), :] = dx[8 * half : 8 * half + 8]
        return carry

    lax.fori_loop(0, 16, prologue, 0)

    BP[...] = jnp.zeros((128, T), F32)
    BP[0:NS] = b_ref[...]
    BP[NS : 2 * NS] = c_ref[...]
    for tb in range(2):
        BTN[128 * tb : 128 * tb + 128, :] = BP[:, 128 * tb : 128 * tb + 128].T
    for i in range(STEPS):
        BTP[8 * i : 8 * i + 8, :] = BTN[pl.ds(i, 8, stride=STEPS), :]
    bt = BTP[...]
    hi = bt.astype(BF16)
    lo = (bt - hi.astype(F32)).astype(BF16)
    bt2 = jnp.concatenate([hi, lo], axis=1)

    def spread(g, carry):
        row = lax.broadcasted_iota(jnp.int32, (256, 512), 0) % 128
        col = lax.broadcasted_iota(jnp.int32, (256, 512), 1) // 128
        pick = jnp.where(row == col + 4 * g, 1.0, 0.0).astype(BF16)
        BB[g] = jnp.dot(bt2, pick, preferred_element_type=F32)
        return carry

    lax.fori_loop(0, 8, spread, 0)

    run = lax.broadcasted_iota(jnp.int32, (8, 128), 0)
    ones8 = jnp.ones((8, 128), F32)

    def roll(v, k):
        return pltpu.roll(v, k, axis=0)

    for j in range(3):
        total = D[j * T : j * T + 8, :]
        for i in range(1, STEPS):
            total = total + D[j * T + 8 * i : j * T + 8 * i + 8, :]
        upto = total
        for k in (1, 2, 4):
            upto = upto + jnp.where(run >= k, roll(upto, k), 0.0)
        CS[0, j] = total
        CS[1, j] = jnp.where(run >= 1, roll(upto, 1), 0.0)
        whole = jnp.broadcast_to(upto[7:8], (8, 128))
        CS[2, j] = whole - upto
        XF[s, j, NS : NS + 8, :] = whole

    def tiles(ref, ng):
        return [ref[ng, 8 * tt : 8 * tt + 8, :] for tt in range(12)]

    def at_step(ref, i):
        return [ref[pl.ds(pl.multiple_of(j * T + 8 * i, 8), 8), :] for j in range(3)]

    def of_states(g, i):
        return [BB[g, pl.ds(pl.multiple_of(8 * i, 8), 8), 128 * nn : 128 * nn + 128] for nn in range(4)]

    def local_forward(ng, carry):
        rates = tiles(A2B, ng)

        def step(i, hs):
            d, dx, b = at_step(D, i), at_step(DX, i), of_states(ng, i)
            new = []
            for tt in range(12):
                nn, j = tt // 3, tt % 3
                dec = jnp.exp2(d[j] * rates[tt])
                DEC[ng, i, 8 * tt : 8 * tt + 8, :] = dec
                new.append(dec * hs[tt] + b[nn] * dx[j])
            return tuple(new)

        ends = lax.fori_loop(0, STEPS, step, (jnp.zeros((8, 128), F32),) * 12, unroll=UNROLL)
        for tt in range(12):
            nn, j = tt // 3, tt % 3
            e, p = ends[tt], jnp.exp2(rates[tt] * CS[0, j])
            for k in (1, 2, 4):
                e = e + jnp.where(run >= k, p * roll(e, k), 0.0)
                p = jnp.where(run >= k, p * roll(p, k), p)
            HPRE[ng, 8 * tt : 8 * tt + 8, :] = jnp.where(run >= 1, roll(e, 1), 0.0)
            XF[s, j, pl.ds(4 * ng + nn, 1), :] = e[7:8]
        return carry

    lax.fori_loop(0, 4, local_forward, 0)

    f_copies = [rc(XF.at[s], XF.at[s], f_send.at[o], f_recv.at[o], (s + o) % 8, c) for o in range(1, 8)]
    for copy in f_copies:
        copy.start()
    for copy in f_copies:
        copy.wait_recv()

    def fold(table, reverse):
        for j in range(3):
            state = jnp.zeros((NS, 128), F32)
            for q in reversed(range(8)) if reverse else range(8):
                here = jnp.full((NS, 128), s, jnp.int32)
                valid = here < q if reverse else here > q
                dec = jnp.exp2(A2N[j] * XF[q, j, NS : NS + 1, :])
                state = jnp.where(valid, dec * state + table[q, j, :NS, :], state)
            HIN[j] = state

    fold(XF, False)

    def forward(ng, carry):
        rates = tiles(A2B, ng)
        hs = []
        for tt in range(12):
            nn, j = tt // 3, tt % 3
            begin = jnp.broadcast_to(HIN[j, pl.ds(4 * ng + nn, 1), :], (8, 128))
            h = HPRE[ng, 8 * tt : 8 * tt + 8, :] + jnp.exp2(rates[tt] * CS[1, j]) * begin
            HS[ng, 0, 8 * tt : 8 * tt + 8, :] = h
            hs.append(h)

        def step(i, hs):
            dx, b, cc = at_step(DX, i), of_states(ng, i), of_states(ng + 4, i)
            new, ys = [], [None] * 3
            for tt in range(12):
                nn, j = tt // 3, tt % 3
                dec = DEC[ng, i, 8 * tt : 8 * tt + 8, :]
                h = dec * hs[tt] + b[nn] * dx[j]
                HS[ng, i + 1, 8 * tt : 8 * tt + 8, :] = h
                ys[j] = cc[nn] * h if nn == 0 else ys[j] + cc[nn] * h
                new.append(h)
            for j in range(3):
                row = pl.ds(pl.multiple_of(j * T + 8 * i, 8), 8)
                Y[row, :] = Y[row, :] + ys[j]
            return tuple(new)

        lax.fori_loop(0, STEPS, step, tuple(hs), unroll=UNROLL)
        return carry

    Y[...] = jnp.zeros_like(Y)
    lax.fori_loop(0, 4, forward, 0)

    def natural(ref, m, j):
        return jnp.concatenate([ref[perm(m, 0, j), :], ref[perm(m, 1, j), :]], axis=0)

    def gate(m, carry):
        rows = pl.ds(pl.multiple_of(16 * m, 16), 16)
        for j in range(3):
            y = natural(Y, m, j) + SKP[0:1, lanes(j)] * XP[rows, lanes(j)].astype(F32)
            z = ZP[rows, lanes(j)].astype(F32)
            YN[rows, lanes(j)] = y
            GF[rows, lanes(j)] = y * z * sigmoid(z)
        return carry

    lax.fori_loop(0, 16, gate, 0)
    for j in range(3):
        for tb in range(2):
            cut = slice(128 * tb, 128 * tb + 128)
            GT[lanes(j), cut] = GF[cut, lanes(j)].T.astype(BF16)
    gt_copy = rc(GT.at[pl.ds(0, E)], GTP, p_send.at[4], p_recv.at[4], partner, c)
    gt_copy.start()

    w_copy.wait()
    for copy in gathers:
        copy.wait_recv()
    swaps = []
    for q in range(4):
        theirs = pl.ds(pl.multiple_of((2 * q + 1 - kap) * 2 * FEAT, 64), 2 * FEAT)
        swaps.append(rc(G.at[theirs], GP.at[q], p_send.at[q], p_recv.at[q], partner, c))
    for copy in swaps:
        copy.start()
    DGT[E:, :] = jnp.zeros((PAD - E, T), F32)
    DGT[:E, :] = jnp.dot(W[...], G[...], preferred_element_type=F32)
    for j in range(3):
        for tb in range(2):
            cut = slice(128 * tb, 128 * tb + 128)
            DG[cut, lanes(j)] = DGT[lanes(j), cut].T

    def ungate(m, sums):
        rows = pl.ds(pl.multiple_of(16 * m, 16), 16)
        new = []
        for j in range(3):
            z, dg = ZP[rows, lanes(j)].astype(F32), DG[rows, lanes(j)]
            sig = sigmoid(z)
            dy = dg * z * sig
            out = (dg * YN[rows, lanes(j)] * sig * (1.0 + z * (1.0 - sig))).astype(BF16)
            if j < 2:
                gg_ref[rows, lanes(j)] = out
            else:
                gg_ref[rows, 256:E] = out[:, : E - 256]
            for half in range(2):
                DY[perm(m, half, j), :] = dy[8 * half : 8 * half + 8]
            prod = dy * XP[rows, lanes(j)].astype(F32)
            new.append(sums[j] + prod[:8] + prod[8:])
        return tuple(new)

    skips = lax.fori_loop(0, 16, ungate, (jnp.zeros((8, 128), F32),) * 3)
    for j in range(3):
        XR[s, j, NS : NS + 8, :] = jnp.broadcast_to(jnp.sum(skips[j], axis=0, keepdims=True), (8, 128))

    def local_adjoint(ng, carry):
        def step(k, oms):
            i = STEPS - 1 - k
            dy, cc = at_step(DY, i), of_states(ng + 4, i)
            new, read = [], [None] * 4
            for tt in range(12):
                nn, j = tt // 3, tt % 3
                lam = cc[nn] * dy[j] + oms[tt]
                new.append(DEC[ng, i, 8 * tt : 8 * tt + 8, :] * lam)
                term = dy[j] * HS[ng, i + 1, 8 * tt : 8 * tt + 8, :]
                read[nn] = term if j == 0 else read[nn] + term
            for nn in range(4):
                PW[1, i, pl.ds(pl.multiple_of(32 * ng, 8) + 8 * nn, 8), :] = read[nn]
            return tuple(new)

        outs = lax.fori_loop(0, STEPS, step, (jnp.zeros((8, 128), F32),) * 12, unroll=UNROLL)
        rates = tiles(A2B, ng)
        for tt in range(12):
            nn, j = tt // 3, tt % 3
            e, p = outs[tt], jnp.exp2(rates[tt] * CS[0, j])
            for k in (1, 2, 4):
                e = e + jnp.where(run < 8 - k, p * roll(e, 8 - k), 0.0)
                p = jnp.where(run < 8 - k, p * roll(p, 8 - k), p)
            HPRE[ng, 8 * tt : 8 * tt + 8, :] = jnp.where(run < 7, roll(e, 7), 0.0)
            XB[s, j, pl.ds(4 * ng + nn, 1), :] = e[0:1]
        return carry

    lax.fori_loop(0, 4, local_adjoint, 0)
    b_copies = [rc(XB.at[s], XB.at[s], b_send.at[o], b_recv.at[o], (s + o) % 8, c) for o in range(1, 8)]
    for copy in b_copies:
        copy.start()

    gt_copy.wait_recv()
    for copy in swaps:
        copy.wait_recv()

    def weight_block(o):
        dest = (chip + o) % 4
        mine = G[pl.ds(pl.multiple_of((2 * dest + kap) * 2 * FEAT, 64), 2 * FEAT), :]
        dims = (((1,), (1,)), ((), ()))
        return lax.dot_general(GT[:E, :], mine, dims, preferred_element_type=F32) + lax.dot_general(
            GTP[...], GP[dest], dims, preferred_element_type=F32
        )

    half = E // 2
    SB[2, :, :E] = weight_block(2).astype(BF16)
    n_copies = [
        rc(SB.at[2, pl.ds(0, half)], RB.at[0], n_send.at[0], n_recv.at[0], up, c),
        rc(SB.at[2, pl.ds(half, half)], RB.at[1], n_send.at[1], n_recv.at[1], down, c),
    ]
    for copy in n_copies:
        copy.start()
    PB[0] = weight_block(1)
    PB[1] = weight_block(3)
    SB[0, half:, :E] = PB[0, half:, :].astype(BF16)
    SB[1, :half, :E] = PB[1, :half, :].astype(BF16)
    PB[2] = weight_block(0)
    late = [
        rc(SB.at[0, pl.ds(half, half)], RB.at[3], n_send.at[2], n_recv.at[2], up, c),
        rc(SB.at[1, pl.ds(0, half)], RB.at[4], n_send.at[3], n_recv.at[3], down, c),
    ]
    for copy in late:
        copy.start()

    for copy in b_copies:
        copy.wait_recv()
    fold(XB, True)

    for copy in n_copies:
        copy.wait_recv()
    SB[0, :half, :E] = (PB[0, :half, :] + RB[0, :, :E].astype(F32)).astype(BF16)
    SB[1, half:, :E] = (PB[1, half:, :] + RB[1, :, :E].astype(F32)).astype(BF16)

    def adjoint(ng, carry):
        rates = tiles(A2B, ng)
        oms = []
        for tt in range(12):
            nn, j = tt // 3, tt % 3
            begin = jnp.broadcast_to(HIN[j, pl.ds(4 * ng + nn, 1), :], (8, 128))
            oms.append(HPRE[ng, 8 * tt : 8 * tt + 8, :] + jnp.exp2(rates[tt] * CS[2, j]) * begin)

        def step(k, state):
            i = STEPS - 1 - k
            oms, accs = state
            d, dx, dy = at_step(D, i), at_step(DX, i), at_step(DY, i)
            b, cc = of_states(ng, i), of_states(ng + 4, i)
            new, acc = [], []
            lb, gd, write = [None] * 3, [None] * 3, [None] * 4
            for tt in range(12):
                nn, j = tt // 3, tt % 3
                lam = cc[nn] * dy[j] + oms[tt]
                om = DEC[ng, i, 8 * tt : 8 * tt + 8, :] * lam
                w = om * HS[ng, i, 8 * tt : 8 * tt + 8, :]
                new.append(om)
                acc.append(accs[tt] + w * d[j])
                lb[j] = lam * b[nn] if nn == 0 else lb[j] + lam * b[nn]
                gd[j] = w * rates[tt] if nn == 0 else gd[j] + w * rates[tt]
                write[nn] = lam * dx[j] if j == 0 else write[nn] + lam * dx[j]
            for nn in range(4):
                PW[0, i, pl.ds(pl.multiple_of(32 * ng, 8) + 8 * nn, 8), :] = write[nn]
            for j in range(3):
                row = pl.ds(pl.multiple_of(j * T + 8 * i, 8), 8)
                LB[row, :] = LB[row, :] + lb[j]
                GD[row, :] = GD[row, :] + gd[j]
            return tuple(new), tuple(acc)

        zeros = (jnp.zeros((8, 128), F32),) * 12
        _, accs = lax.fori_loop(0, STEPS, step, (tuple(oms), zeros), unroll=UNROLL)
        for tt in range(12):
            nn, j = tt // 3, tt % 3
            total = jnp.sum(accs[tt], axis=0, keepdims=True)
            XR[s, j, pl.ds(4 * ng + nn, 1), :] = LN2 * total * rates[tt][0:1]
        return carry

    LB[...] = jnp.zeros_like(LB)
    GD[...] = jnp.zeros_like(GD)
    final = [
        rc(SB.at[0, pl.ds(0, half)], RB.at[2], n_send.at[4], n_recv.at[4], up, c),
        rc(SB.at[1, pl.ds(half, half)], RB.at[5], n_send.at[5], n_recv.at[5], down, c),
    ]
    for copy in final:
        copy.start()
    lax.fori_loop(0, 4, adjoint, 0)
    r_copies = [rc(XR.at[s], XR.at[s], r_send.at[o], r_recv.at[o], (s + o) % 8, c) for o in range(1, 8)]
    for copy in r_copies:
        copy.start()

    def lane_sums(i, acc):
        col = lax.broadcasted_iota(jnp.int32, (256, 128), 1)
        row = lax.broadcasted_iota(jnp.int32, (256, 128), 0) // 128
        pick = jnp.where(col == i + 32 * row, 1.0, 0.0).astype(BF16)
        both = jnp.concatenate([PW[0, i], PW[1, i]], axis=1).astype(BF16)
        return acc + jnp.dot(both, pick, preferred_element_type=F32)

    sums = lax.fori_loop(0, STEPS, lane_sums, jnp.zeros((128, 128), F32), unroll=4)
    for n in range(NS):
        R2[pl.ds(n, 8, stride=NS), :] = sums[8 * n : 8 * n + 8]

    def x_rows(dest):
        return pl.ds(pl.multiple_of((dest // 2) * NS, NS), NS)

    x_copies = [
        rc(R2.at[x_rows((c + o) % 16)], GX.at[o], x_send.at[o], x_recv.at[o], s, (c + o) % 16)
        for o in range(1, 16)
    ]
    for copy in x_copies:
        copy.start()

    def epilogue(m, carry):
        rows = pl.ds(pl.multiple_of(16 * m, 16), 16)
        for j in range(3):
            x, st = XP[rows, lanes(j)].astype(F32), TP[rows, lanes(j)].astype(F32)
            lb = natural(LB, m, j)
            gi = (natural(D, m, j) * lb + natural(DY, m, j) * SKP[0:1, lanes(j)]).astype(BF16)
            gs = ((x * lb + LN2 * natural(GD, m, j)) * sigmoid(st)).astype(BF16)
            if j < 2:
                gi_ref[rows, lanes(j)] = gi
                gs_ref[rows, lanes(j)] = gs
            else:
                gi_ref[rows, 256:E] = gi[:, : E - 256]
                gs_ref[rows, 256:E] = gs[:, : E - 256]
        return carry

    lax.fori_loop(0, 16, epilogue, 0)

    for copy in r_copies:
        copy.wait_recv()
    for j in range(3):
        total = XR[0, j]
        for q in range(1, 8):
            total = total + XR[q, j]
        wide = 128 if j < 2 else E - 256
        gr_ref[:, 128 * j : 128 * j + wide] = total[:NS, :wide]
        gk_ref[:, 128 * j : 128 * j + wide] = total[NS : NS + 1, :wide]

    for copy in late + final:
        copy.wait_recv()
    gw_ref[:half, :] = PB[2, :half, :] + RB[2, :, :E].astype(F32) + RB[4, :, :E].astype(F32)
    gw_ref[half:, :] = PB[2, half:, :] + RB[3, :, :E].astype(F32) + RB[5, :, :E].astype(F32)

    for copy in x_copies:
        copy.wait_recv()
    mine = R2[x_rows(c), :]
    for o in range(1, 16):
        mine = mine + GX[o]
    odd = jnp.full((NS, NS), c % 2, jnp.int32) == 1
    gwrite_ref[...] = jnp.where(odd, mine[:, 16:32], mine[:, 0:16])
    gread_ref[...] = jnp.where(odd, mine[:, 48:64], mine[:, 32:48])

    for copy in gathers + f_copies + swaps + [gt_copy] + b_copies + n_copies + late + final + r_copies + x_copies:
        copy.wait_send()


SCRATCH = dict(
    W=((E, DM), BF16), G=((DM, T), BF16), GP=((4, 2 * FEAT, T), BF16), DOP=((T, 256), BF16),
    XP=((T, PAD), BF16), ZP=((T, PAD), BF16), TP=((T, PAD), BF16), SKP=((8, PAD), F32), LRP=((NS, PAD), F32),
    A2N=((3, NS, 128), F32), A2B=((4, 96, 128), F32), BP=((128, T), F32), BTN=((T, 128), F32), BTP=((T, 128), F32),
    BB=((8, T, 512), F32), D=((3 * T, 128), F32), DX=((3 * T, 128), F32), DY=((3 * T, 128), F32),
    Y=((3 * T, 128), F32), LB=((3 * T, 128), F32), GD=((3 * T, 128), F32),
    DEC=((4, STEPS, 96, 128), F32), HS=((4, STEPS + 1, 96, 128), F32), HPRE=((4, 96, 128), F32),
    HIN=((3, NS, 128), F32), PW=((2, STEPS, 128, 128), F32), CS=((3, 3, 8, 128), F32),
    YN=((T, PAD), F32), GF=((T, PAD), F32), GT=((PAD, T), BF16), GTP=((E, T), BF16),
    DGT=((PAD, T), F32), DG=((T, PAD), F32), PB=((3, E, E), F32), SB=((3, E, PAD), BF16), RB=((6, E // 2, PAD), BF16),
    XF=((8, 3, 24, 128), F32), XB=((8, 3, NS, 128), F32), XR=((8, 3, 24, 128), F32),
    R2=((128, 128), F32), GX=((16, NS, 128), F32),
)
SEMS = (None, 16, 16, 5, 5, 8, 8, 8, 8, 8, 8, 6, 6, 16, 16)


def on_device(x, z, st, lr, sk, b, c, w, do):
    vmem, shape = pl.BlockSpec(memory_space=pltpu.VMEM), jax.ShapeDtypeStruct
    dma = pltpu.SemaphoreType.DMA
    outs = pl.pallas_call(
        kernel,
        out_shape=(
            shape((T, E), BF16), shape((T, E), BF16), shape((T, E), BF16), shape((NS, E), F32), shape((1, E), F32),
            shape((NS, NS), F32), shape((NS, NS), F32), shape((E, E), F32),
        ),
        in_specs=[vmem] * 7 + [pl.BlockSpec(memory_space=pl.ANY), vmem],
        out_specs=(vmem,) * 8,
        scratch_shapes=[pltpu.VMEM(*v) for v in SCRATCH.values()] + [dma if n is None else dma((n,)) for n in SEMS],
        compiler_params=pltpu.CompilerParams(
            collective_id=0, has_side_effects=True, vmem_limit_bytes=60 * 1024 * 1024
        ),
    )(x, z, st, lr, sk.reshape(1, E), b, c, w, do)
    return outs[:4] + (outs[4].reshape(E),) + outs[5:]


def solution(mesh):
    return jax.shard_map(
        on_device,
        mesh=mesh,
        in_specs=(
            P("seq", "chan"), P("seq", "chan"), P("seq", "chan"), P(None, "chan"), P("chan"),
            P(None, "seq"), P(None, "seq"), P("chan", None), P("seq", "chan"),
        ),
        out_specs=(
            P("seq", "chan"), P("seq", "chan"), P("seq", "chan"), P(None, "chan"), P("chan"),
            P(None, ("seq", "chan")), P(None, ("seq", "chan")), P("chan", "seq"),
        ),
        check_vma=False,
    )
```

```python
import math

import jax
import jax.numpy as jnp
from jax import lax
from jax.experimental import pallas as pl
from jax.experimental.pallas import tpu as pltpu
from jax.sharding import PartitionSpec as P

F32, BF16 = jnp.float32, jnp.bfloat16
LOG2E, LN2 = 1.0 / math.log(2.0), math.log(2.0)
T, E, PAD, NS, DM = 256, 320, 384, 16, 2560
SUB, STEPS = 8, 32
FEAT = 160
UNROLL = 2


def sigmoid(v):
    return 1.0 / (1.0 + jnp.exp(-v))


class Phases:
    def __init__(self):
        self.now = None

    def __call__(self, name):
        if self.now is not None:
            self.now.__exit__(None, None, None)
        self.now = jax.named_scope(name) if name else None
        if self.now is not None:
            self.now.__enter__()


def kernel(
    x_ref, z_ref, st_ref, lr_ref, sk_ref, b_ref, c_ref, w_hbm, do_ref,
    gi_hbm, gg_hbm, gs_hbm, gr_hbm, gk_hbm, gwrite_hbm, gread_hbm, gw_hbm,
    gi_ref, gg_ref, gs_ref, gr_ref, gk_ref, gwrite_ref, gread_ref, gw_ref,
    W, G, GP, SKB, LRP, A2N, A2B, BP, BTN, BTP, BB, DT, DXT, D, DX, DY, Y, LB, GD,
    DEC, HS, HPRE, HIN, PW, CS, YT, GDT, SILU, GT, GTP, PB, SB, RB, XF, XB, XR, R2, GX,
    w_sem, o_sem, g_send, g_recv, p_send, p_recv, f_send, f_recv, b_send, b_recv, r_send, r_recv,
    n_send, n_recv, x_send, x_recv,
):
    phase = Phases()
    phase("enter")
    s, c = lax.axis_index("seq"), lax.axis_index("chan")
    kap, chip = s % 2, s // 2
    partner = s + 1 - 2 * kap
    up, down = ((chip + 1) % 4) * 2 + kap, ((chip + 3) % 4) * 2 + kap

    def rc(src, dst, ss, rs, ps, pc):
        return pltpu.make_async_remote_copy(
            src_ref=src, dst_ref=dst, send_sem=ss, recv_sem=rs,
            device_id=(ps, pc), device_id_type=pl.DeviceIdType.MESH,
        )

    w_copy = pltpu.make_async_copy(w_hbm, W, w_sem)
    w_copy.start()
    barrier = pltpu.get_barrier_semaphore()
    for o in range(1, 16):
        pl.semaphore_signal(barrier, inc=1, device_id=(s, (c + o) % 16), device_id_type=pl.DeviceIdType.MESH)
    for o in range(1, 8):
        pl.semaphore_signal(barrier, inc=1, device_id=((s + o) % 8, c), device_id_type=pl.DeviceIdType.MESH)

    own = pl.multiple_of(c * FEAT, 32)
    G[pl.ds(own, FEAT), :] = do_ref[...]
    pl.semaphore_wait(barrier, 22)

    def g_copy(o):
        q = pl.ds(own, FEAT)
        return rc(do_ref, G.at[q], g_send.at[o], g_recv.at[o], s, (c + o) % 16)

    gathers = [g_copy(o) for o in range(1, 16)]
    for copy in gathers:
        copy.start()

    phase("prologue")
    LRP[:, 256:] = jnp.zeros((NS, 128), F32)
    LRP[:, :E] = lr_ref[...]
    for j in range(3):
        A2N[j] = -LOG2E * jnp.exp(LRP[:, 128 * j : 128 * j + 128])
    for n in range(NS):
        for j in range(3):
            tt = (n % 4) * 3 + j
            A2B[n // 4, 8 * tt : 8 * tt + 8, :] = jnp.broadcast_to(A2N[j, n : n + 1, :], (8, 128))
    LRP[0:1, :E] = sk_ref[...].reshape(1, E)
    for j in range(3):
        SKB[128 * j : 128 * j + 128, :] = jnp.broadcast_to(LRP[0:1, 128 * j : 128 * j + 128], (128, 128)).T

    def lanes(j):
        return slice(128 * j, 128 * j + 128)

    def block(m):
        return pl.ds(pl.multiple_of(16 * m, 16), 16)

    def prologue(m, carry):
        rows = block(m)
        st = st_ref[rows, :].astype(F32)
        delta = jnp.maximum(st, 0.0) + jnp.log1p(jnp.exp(-jnp.abs(st)))
        DT[rows, :] = delta
        DXT[rows, :] = delta * x_ref[rows, :].astype(F32)
        return carry

    DT[E:, :] = jnp.zeros((PAD - E, T), F32)
    DXT[E:, :] = jnp.zeros((PAD - E, T), F32)
    lax.fori_loop(0, E // 16, prologue, 0, unroll=2)

    def places():
        for j in range(3):
            for tb in range(2):
                at = [pl.ds(j * T + 8 * (8 * (q % 4)) + 4 * tb + q // 4, 8, stride=8) for q in range(16)]
                yield lanes(j), lanes(tb), at

    def by_step(src, dst):
        for rows, cols, at in places():
            turned = src[rows, cols].T
            for q in range(16):
                dst[at[q], :] = turned[8 * q : 8 * q + 8]

    def by_channel(src, dst):
        for rows, cols, at in places():
            dst[rows, cols] = jnp.concatenate([src[at[q], :] for q in range(16)], axis=0).T

    by_step(DT, D)
    by_step(DXT, DX)

    phase("spread")
    BP[...] = jnp.zeros((128, T), F32)
    BP[0:NS] = b_ref[...]
    BP[NS : 2 * NS] = c_ref[...]
    for tb in range(2):
        BTN[128 * tb : 128 * tb + 128, :] = BP[:, 128 * tb : 128 * tb + 128].T
    for i in range(STEPS):
        BTP[8 * i : 8 * i + 8, :] = BTN[pl.ds(i, 8, stride=STEPS), :]
    bt = BTP[...]
    hi = bt.astype(BF16)
    lo = (bt - hi.astype(F32)).astype(BF16)
    bt2 = jnp.concatenate([hi, lo], axis=1)

    def spread(g, carry):
        row = lax.broadcasted_iota(jnp.int32, (256, 512), 0) % 128
        col = lax.broadcasted_iota(jnp.int32, (256, 512), 1) // 128
        pick = jnp.where(row == col + 4 * g, 1.0, 0.0).astype(BF16)
        BB[g] = jnp.dot(bt2, pick, preferred_element_type=F32)
        return carry

    lax.fori_loop(0, 8, spread, 0)

    run = lax.broadcasted_iota(jnp.int32, (8, 128), 0)
    ones8 = jnp.ones((8, 128), F32)

    def roll(v, k):
        return pltpu.roll(v, k, axis=0)

    for j in range(3):
        total = D[j * T : j * T + 8, :]
        for i in range(1, STEPS):
            total = total + D[j * T + 8 * i : j * T + 8 * i + 8, :]
        upto = total
        for k in (1, 2, 4):
            upto = upto + jnp.where(run >= k, roll(upto, k), 0.0)
        CS[0, j] = total
        CS[1, j] = jnp.where(run >= 1, roll(upto, 1), 0.0)
        whole = jnp.broadcast_to(upto[7:8], (8, 128))
        CS[2, j] = whole - upto
        XF[s, j, NS : NS + 8, :] = whole

    def tiles(ref, ng):
        return [ref[ng, 8 * tt : 8 * tt + 8, :] for tt in range(12)]

    def at_step(ref, i):
        return [ref[pl.ds(pl.multiple_of(j * T + 8 * i, 8), 8), :] for j in range(3)]

    def of_states(g, i):
        return [BB[g, pl.ds(pl.multiple_of(8 * i, 8), 8), 128 * nn : 128 * nn + 128] for nn in range(4)]

    phase("pass1")
    def local_forward(ng, carry):
        rates = tiles(A2B, ng)

        def step(i, hs):
            d, dx, b = at_step(D, i), at_step(DX, i), of_states(ng, i)
            new = []
            for tt in range(12):
                nn, j = tt // 3, tt % 3
                dec = jnp.exp2(d[j] * rates[tt])
                DEC[ng, i, 8 * tt : 8 * tt + 8, :] = dec
                new.append(dec * hs[tt] + b[nn] * dx[j])
            return tuple(new)

        ends = lax.fori_loop(0, STEPS, step, (jnp.zeros((8, 128), F32),) * 12, unroll=UNROLL)
        for tt in range(12):
            nn, j = tt // 3, tt % 3
            e, p = ends[tt], jnp.exp2(rates[tt] * CS[0, j])
            for k in (1, 2, 4):
                e = e + jnp.where(run >= k, p * roll(e, k), 0.0)
                p = jnp.where(run >= k, p * roll(p, k), p)
            HPRE[ng, 8 * tt : 8 * tt + 8, :] = jnp.where(run >= 1, roll(e, 1), 0.0)
            XF[s, j, pl.ds(4 * ng + nn, 1), :] = e[7:8]
        return carry

    lax.fori_loop(0, 4, local_forward, 0)

    phase("fexchange")
    f_copies = [rc(XF.at[s], XF.at[s], f_send.at[o], f_recv.at[o], (s + o) % 8, c) for o in range(1, 8)]
    for copy in f_copies:
        copy.start()
    for copy in f_copies:
        copy.wait_recv()

    def fold(table, reverse):
        for j in range(3):
            state = jnp.zeros((NS, 128), F32)
            for q in reversed(range(8)) if reverse else range(8):
                here = jnp.full((NS, 128), s, jnp.int32)
                valid = here < q if reverse else here > q
                dec = jnp.exp2(A2N[j] * XF[q, j, NS : NS + 1, :])
                state = jnp.where(valid, dec * state + table[q, j, :NS, :], state)
            HIN[j] = state

    fold(XF, False)

    phase("pass2")
    def forward(ng, carry):
        rates = tiles(A2B, ng)
        hs = []
        for tt in range(12):
            nn, j = tt // 3, tt % 3
            begin = jnp.broadcast_to(HIN[j, pl.ds(4 * ng + nn, 1), :], (8, 128))
            h = HPRE[ng, 8 * tt : 8 * tt + 8, :] + jnp.exp2(rates[tt] * CS[1, j]) * begin
            HS[ng, 0, 8 * tt : 8 * tt + 8, :] = h
            hs.append(h)

        def step(i, hs):
            dx, b, cc = at_step(DX, i), of_states(ng, i), of_states(ng + 4, i)
            new, ys = [], [None] * 3
            for tt in range(12):
                nn, j = tt // 3, tt % 3
                dec = DEC[ng, i, 8 * tt : 8 * tt + 8, :]
                h = dec * hs[tt] + b[nn] * dx[j]
                HS[ng, i + 1, 8 * tt : 8 * tt + 8, :] = h
                ys[j] = cc[nn] * h if nn == 0 else ys[j] + cc[nn] * h
                new.append(h)
            for j in range(3):
                row = pl.ds(pl.multiple_of(j * T + 8 * i, 8), 8)
                Y[row, :] = Y[row, :] + ys[j]
            return tuple(new)

        lax.fori_loop(0, STEPS, step, tuple(hs), unroll=UNROLL)
        return carry

    Y[...] = jnp.zeros_like(Y)
    lax.fori_loop(0, 4, forward, 0)

    phase("gate")
    by_channel(Y, YT)

    def gate(m, carry):
        rows = block(m)
        skip = SKB[rows, :]
        y = YT[rows, :] + jnp.concatenate([skip, skip], axis=1) * x_ref[rows, :].astype(F32)
        z = z_ref[rows, :].astype(F32)
        sig = sigmoid(z)
        SILU[rows, :] = z * sig
        GT[rows, :] = (y * z * sig).astype(BF16)
        YT[rows, :] = y * sig * (1.0 + z * (1.0 - sig))
        return carry

    lax.fori_loop(0, E // 16, gate, 0, unroll=2)
    gt_copy = rc(GT, GTP, p_send.at[4], p_recv.at[4], partner, c)
    gt_copy.start()

    phase("gwait")
    w_copy.wait()
    for copy in gathers:
        copy.wait_recv()
    swaps = []
    for q in range(4):
        theirs = pl.ds(pl.multiple_of((2 * q + 1 - kap) * 2 * FEAT, 64), 2 * FEAT)
        swaps.append(rc(G.at[theirs], GP.at[q], p_send.at[q], p_recv.at[q], partner, c))
    for copy in swaps:
        copy.start()
    phase("dg")
    for j in range(3):
        rows = slice(128 * j, min(128 * j + 128, E))
        dg = jnp.dot(W[rows, :], G[...], preferred_element_type=F32)
        dy = dg * SILU[rows, :]
        DXT[rows, :] = dy
        gg_ref[rows, :] = (dg * YT[rows, :]).astype(BF16)
        SILU[rows, :] = dy * x_ref[rows, :].astype(F32)
    gg_out = pltpu.make_async_copy(gg_ref, gg_hbm, o_sem.at[1])
    gg_out.start()
    by_step(DXT, DY)
    ones = jnp.ones((8, T), BF16)
    skips = lax.dot_general(ones, SILU[...].astype(BF16), (((1,), (1,)), ((), ())), preferred_element_type=F32)
    for j in range(3):
        wide = 128 if j < 2 else E - 256
        if j == 2:
            XR[s, j, NS : NS + 8, :] = jnp.zeros((8, 128), F32)
        XR[s, j, NS : NS + 8, :wide] = skips[:, 128 * j : 128 * j + wide]

    phase("pass3")
    def local_adjoint(ng, carry):
        def step(k, oms):
            i = STEPS - 1 - k
            dy, cc = at_step(DY, i), of_states(ng + 4, i)
            new, read = [], [None] * 4
            for tt in range(12):
                nn, j = tt // 3, tt % 3
                lam = cc[nn] * dy[j] + oms[tt]
                new.append(DEC[ng, i, 8 * tt : 8 * tt + 8, :] * lam)
                term = dy[j] * HS[ng, i + 1, 8 * tt : 8 * tt + 8, :]
                read[nn] = term if j == 0 else read[nn] + term
            for nn in range(4):
                PW[1, i, pl.ds(pl.multiple_of(32 * ng, 8) + 8 * nn, 8), :] = read[nn]
            return tuple(new)

        outs = lax.fori_loop(0, STEPS, step, (jnp.zeros((8, 128), F32),) * 12, unroll=UNROLL)
        rates = tiles(A2B, ng)
        for tt in range(12):
            nn, j = tt // 3, tt % 3
            e, p = outs[tt], jnp.exp2(rates[tt] * CS[0, j])
            for k in (1, 2, 4):
                e = e + jnp.where(run < 8 - k, p * roll(e, 8 - k), 0.0)
                p = jnp.where(run < 8 - k, p * roll(p, 8 - k), p)
            HPRE[ng, 8 * tt : 8 * tt + 8, :] = jnp.where(run < 7, roll(e, 7), 0.0)
            XB[s, j, pl.ds(4 * ng + nn, 1), :] = e[0:1]
        return carry

    lax.fori_loop(0, 4, local_adjoint, 0)
    phase("weight")
    b_copies = [rc(XB.at[s], XB.at[s], b_send.at[o], b_recv.at[o], (s + o) % 8, c) for o in range(1, 8)]
    for copy in b_copies:
        copy.start()

    gt_copy.wait_recv()
    for copy in swaps:
        copy.wait_recv()

    def weight_block(o):
        dest = (chip + o) % 4
        mine = G[pl.ds(pl.multiple_of((2 * dest + kap) * 2 * FEAT, 64), 2 * FEAT), :]
        dims = (((1,), (1,)), ((), ()))
        return lax.dot_general(GT[...], mine, dims, preferred_element_type=F32) + lax.dot_general(
            GTP[...], GP[dest], dims, preferred_element_type=F32
        )

    half = E // 2
    SB[2, :, :E] = weight_block(2).astype(BF16)
    n_copies = [
        rc(SB.at[2, pl.ds(0, half)], RB.at[0], n_send.at[0], n_recv.at[0], up, c),
        rc(SB.at[2, pl.ds(half, half)], RB.at[1], n_send.at[1], n_recv.at[1], down, c),
    ]
    for copy in n_copies:
        copy.start()
    PB[0] = weight_block(1)
    PB[1] = weight_block(3)
    SB[0, half:, :E] = PB[0, half:, :].astype(BF16)
    SB[1, :half, :E] = PB[1, :half, :].astype(BF16)
    PB[2] = weight_block(0)
    late = [
        rc(SB.at[0, pl.ds(half, half)], RB.at[3], n_send.at[2], n_recv.at[2], up, c),
        rc(SB.at[1, pl.ds(0, half)], RB.at[4], n_send.at[3], n_recv.at[3], down, c),
    ]
    for copy in late:
        copy.start()

    phase("bwait")
    for copy in b_copies:
        copy.wait_recv()
    fold(XB, True)

    phase("nwait")
    for copy in n_copies:
        copy.wait_recv()
    SB[0, :half, :E] = (PB[0, :half, :] + RB[0, :, :E].astype(F32)).astype(BF16)
    SB[1, half:, :E] = (PB[1, half:, :] + RB[1, :, :E].astype(F32)).astype(BF16)

    phase("pass4")
    def adjoint(ng, carry):
        rates = tiles(A2B, ng)
        oms = []
        for tt in range(12):
            nn, j = tt // 3, tt % 3
            begin = jnp.broadcast_to(HIN[j, pl.ds(4 * ng + nn, 1), :], (8, 128))
            oms.append(HPRE[ng, 8 * tt : 8 * tt + 8, :] + jnp.exp2(rates[tt] * CS[2, j]) * begin)

        def step(k, state):
            i = STEPS - 1 - k
            oms, accs = state
            d, dx, dy = at_step(D, i), at_step(DX, i), at_step(DY, i)
            b, cc = of_states(ng, i), of_states(ng + 4, i)
            new, acc = [], []
            lb, gd, write = [None] * 3, [None] * 3, [None] * 4
            for tt in range(12):
                nn, j = tt // 3, tt % 3
                lam = cc[nn] * dy[j] + oms[tt]
                om = DEC[ng, i, 8 * tt : 8 * tt + 8, :] * lam
                w = om * HS[ng, i, 8 * tt : 8 * tt + 8, :]
                new.append(om)
                acc.append(accs[tt] + w * d[j])
                lb[j] = lam * b[nn] if nn == 0 else lb[j] + lam * b[nn]
                gd[j] = w * rates[tt] if nn == 0 else gd[j] + w * rates[tt]
                write[nn] = lam * dx[j] if j == 0 else write[nn] + lam * dx[j]
            for nn in range(4):
                PW[0, i, pl.ds(pl.multiple_of(32 * ng, 8) + 8 * nn, 8), :] = write[nn]
            for j in range(3):
                row = pl.ds(pl.multiple_of(j * T + 8 * i, 8), 8)
                LB[row, :] = LB[row, :] + lb[j]
                GD[row, :] = GD[row, :] + gd[j]
            return tuple(new), tuple(acc)

        zeros = (jnp.zeros((8, 128), F32),) * 12
        _, accs = lax.fori_loop(0, STEPS, step, (tuple(oms), zeros), unroll=UNROLL)
        for tt in range(12):
            nn, j = tt // 3, tt % 3
            total = jnp.sum(accs[tt], axis=0, keepdims=True)
            XR[s, j, pl.ds(4 * ng + nn, 1), :] = LN2 * total * rates[tt][0:1]
        return carry

    LB[...] = jnp.zeros_like(LB)
    GD[...] = jnp.zeros_like(GD)
    final = [
        rc(SB.at[0, pl.ds(0, half)], RB.at[2], n_send.at[4], n_recv.at[4], up, c),
        rc(SB.at[1, pl.ds(half, half)], RB.at[5], n_send.at[5], n_recv.at[5], down, c),
    ]
    for copy in final:
        copy.start()
    lax.fori_loop(0, 4, adjoint, 0)
    phase("lanesums")
    r_copies = [rc(XR.at[s], XR.at[s], r_send.at[o], r_recv.at[o], (s + o) % 8, c) for o in range(1, 8)]
    for copy in r_copies:
        copy.start()

    def lane_sums(i, acc):
        col = lax.broadcasted_iota(jnp.int32, (256, 128), 1)
        row = lax.broadcasted_iota(jnp.int32, (256, 128), 0) // 128
        pick = jnp.where(col == i + 32 * row, 1.0, 0.0).astype(BF16)
        both = jnp.concatenate([PW[0, i], PW[1, i]], axis=1).astype(BF16)
        return acc + jnp.dot(both, pick, preferred_element_type=F32)

    sums = lax.fori_loop(0, STEPS, lane_sums, jnp.zeros((128, 128), F32), unroll=4)
    for n in range(NS):
        R2[pl.ds(n, 8, stride=NS), :] = sums[8 * n : 8 * n + 8]

    def x_rows(dest):
        return pl.ds(pl.multiple_of((dest // 2) * NS, NS), NS)

    x_copies = [
        rc(R2.at[x_rows((c + o) % 16)], GX.at[o], x_send.at[o], x_recv.at[o], s, (c + o) % 16)
        for o in range(1, 16)
    ]
    for copy in x_copies:
        copy.start()

    phase("epilogue")
    by_channel(LB, YT)
    by_channel(GD, GDT)

    def epilogue(m, carry):
        rows = block(m)
        skip, lb = SKB[rows, :], YT[rows, :]
        dy = DXT[rows, :]
        gi_ref[rows, :] = (DT[rows, :] * lb + dy * jnp.concatenate([skip, skip], axis=1)).astype(BF16)
        gd = x_ref[rows, :].astype(F32) * lb + LN2 * GDT[rows, :]
        gs_ref[rows, :] = (gd * sigmoid(st_ref[rows, :].astype(F32))).astype(BF16)
        return carry

    lax.fori_loop(0, E // 16, epilogue, 0, unroll=2)
    outs = [
        pltpu.make_async_copy(gi_ref, gi_hbm, o_sem.at[0]),
        pltpu.make_async_copy(gs_ref, gs_hbm, o_sem.at[2]),
    ]
    for copy in outs:
        copy.start()

    phase("rwait")
    for copy in r_copies:
        copy.wait_recv()
    for j in range(3):
        total = XR[0, j]
        for q in range(1, 8):
            total = total + XR[q, j]
        wide = 128 if j < 2 else E - 256
        gr_ref[:, 128 * j : 128 * j + wide] = total[:NS, :wide]
        gk_ref[:, 128 * j : 128 * j + wide] = total[NS : NS + 1, :wide]
    phase("gw")

    for copy in late + final:
        copy.wait_recv()
    gw_ref[:half, :] = PB[2, :half, :] + RB[2, :, :E].astype(F32) + RB[4, :, :E].astype(F32)
    gw_ref[half:, :] = PB[2, half:, :] + RB[3, :, :E].astype(F32) + RB[5, :, :E].astype(F32)

    phase("xwait")
    for copy in x_copies:
        copy.wait_recv()
    mine = R2[x_rows(c), :]
    for o in range(1, 16):
        mine = mine + GX[o]
    odd = jnp.full((NS, NS), c % 2, jnp.int32) == 1
    gwrite_ref[...] = jnp.where(odd, mine[:, 16:32], mine[:, 0:16])
    gread_ref[...] = jnp.where(odd, mine[:, 48:64], mine[:, 32:48])

    phase("leave")
    pairs = ((gr_ref, gr_hbm), (gk_ref, gk_hbm), (gwrite_ref, gwrite_hbm), (gread_ref, gread_hbm), (gw_ref, gw_hbm))
    for k, (src, dst) in enumerate(pairs):
        outs.append(pltpu.make_async_copy(src, dst, o_sem.at[3 + k]))
        outs[-1].start()
    for copy in gathers + f_copies + swaps + [gt_copy] + b_copies + n_copies + late + final + r_copies + x_copies:
        copy.wait_send()
    for copy in outs + [gg_out]:
        copy.wait()
    phase(None)


def finish(*refs):
    srcs, dsts, bufs, sems = refs[:8], refs[8:16], refs[16:24], refs[24:]
    ins = [pltpu.make_async_copy(a, v, sems[0].at[k]) for k, (a, v) in enumerate(zip(srcs, bufs))]
    outs = [pltpu.make_async_copy(v, a, sems[1].at[k]) for k, (a, v) in enumerate(zip(dsts, bufs)) if k != 4]
    for copy in ins:
        copy.start()
    for copy in ins:
        copy.wait()
    for copy in outs:
        copy.start()
    dsts[4][...] = bufs[4][...].reshape(E)
    for copy in outs:
        copy.wait()


RESULTS = (
    ((E, T), BF16), ((E, T), BF16), ((E, T), BF16), ((NS, E), F32), ((1, E), F32),
    ((NS, NS), F32), ((NS, NS), F32), ((E, E), F32),
)
SCRATCH = dict(
    W=((E, DM), BF16), G=((DM, T), BF16), GP=((4, 2 * FEAT, T), BF16), SKB=((PAD, 128), F32), LRP=((NS, PAD), F32),
    A2N=((3, NS, 128), F32), A2B=((4, 96, 128), F32), BP=((128, T), F32), BTN=((T, 128), F32), BTP=((T, 128), F32),
    BB=((8, T, 512), F32), DT=((PAD, T), F32), DXT=((PAD, T), F32),
    D=((3 * T, 128), F32), DX=((3 * T, 128), F32), DY=((3 * T, 128), F32),
    Y=((3 * T, 128), F32), LB=((3 * T, 128), F32), GD=((3 * T, 128), F32),
    DEC=((4, STEPS, 96, 128), F32), HS=((4, STEPS + 1, 96, 128), F32), HPRE=((4, 96, 128), F32),
    HIN=((3, NS, 128), F32), PW=((2, STEPS, 128, 128), F32), CS=((3, 3, 8, 128), F32),
    YT=((PAD, T), F32), GDT=((PAD, T), F32), SILU=((E, T), F32), GT=((E, T), BF16), GTP=((E, T), BF16),
    PB=((3, E, E), F32), SB=((3, E, PAD), BF16), RB=((6, E // 2, PAD), BF16),
    XF=((8, 3, 24, 128), F32), XB=((8, 3, NS, 128), F32), XR=((8, 3, 24, 128), F32),
    R2=((128, 128), F32), GX=((16, NS, 128), F32),
)
SEMS = (None, 8, 16, 16, 5, 5, 8, 8, 8, 8, 8, 8, 6, 6, 16, 16)


def on_device(x, z, st, lr, sk, b, c, w, do):
    vmem, hbm = pl.BlockSpec(memory_space=pltpu.VMEM), pl.BlockSpec(memory_space=pl.ANY)
    dma = pltpu.SemaphoreType.DMA
    buffers = [pltpu.VMEM(*v) for v in RESULTS]
    parts = pl.pallas_call(
        kernel,
        out_shape=[jax.ShapeDtypeStruct(*v) for v in RESULTS],
        in_specs=[vmem] * 7 + [hbm, vmem],
        out_specs=[hbm] * 8,
        scratch_shapes=buffers
        + [pltpu.VMEM(*v) for v in SCRATCH.values()]
        + [dma if n is None else dma((n,)) for n in SEMS],
        compiler_params=pltpu.CompilerParams(
            collective_id=0, has_side_effects=True, vmem_limit_bytes=60 * 1024 * 1024
        ),
    )(x.T, z.T, st.T, lr, sk, b, c, w, do.T)
    shapes = [jax.ShapeDtypeStruct(*v) for v in RESULTS]
    shapes[4] = jax.ShapeDtypeStruct((E,), F32)
    specs = [hbm] * 8
    specs[4] = vmem
    outs = pl.pallas_call(
        finish,
        out_shape=shapes,
        in_specs=[hbm] * 8,
        out_specs=specs,
        scratch_shapes=buffers + [dma((8,)), dma((8,))],
    )(*parts)
    return (outs[0].T, outs[1].T, outs[2].T, *outs[3:])


def solution(mesh):
    return jax.shard_map(
        on_device,
        mesh=mesh,
        in_specs=(
            P("seq", "chan"), P("seq", "chan"), P("seq", "chan"), P(None, "chan"), P("chan"),
            P(None, "seq"), P(None, "seq"), P("chan", None), P("seq", "chan"),
        ),
        out_specs=(
            P("seq", "chan"), P("seq", "chan"), P("seq", "chan"), P(None, "chan"), P("chan"),
            P(None, ("seq", "chan")), P(None, ("seq", "chan")), P("chan", "seq"),
        ),
        check_vma=False,
    )
```
